32 devices in a mesh: dp: 8 (over y, x, core), expert: 4 (over z).
Axes of the slice: x: 2, y: 2, z: 4, core: 2. Of those that a mesh axis runs over, the one named last changes fastest.
Arguments:
- out_grad: bfloat16 [64, 4096], P(('dp', 'expert')), may hold values from -0.29882812 to 0.29882812
- routes: int32 [64, 2], P('dp'), may hold values from 0 to 7, all different within a row; in each aligned block of 8 rows (0 to 7, 8 to 15, ...) at most 3 rows name the same one
- gate_values: bfloat16 [64, 2], P(('dp', 'expert')), may hold values from 0.099609375 to 1
- gate_pre: bfloat16 [8, 24, 12288], P('expert', None, 'dp'), may hold values from -6 to 6
- up_pre: bfloat16 [8, 24, 12288], P('expert', None, 'dp'), may hold values from -6 to 6
- w_down: bfloat16 [8, 12288, 4096], P('expert', 'dp'), may hold values from -0.0546875 to 0.0546875
Outputs:
- grad_gates: float32 [64, 2], P(('dp', 'expert'))
- grad_gate_pre: bfloat16 [8, 24, 12288], P('expert', None, 'dp')
- grad_up_pre: bfloat16 [8, 24, 12288], P('expert', None, 'dp')
- grad_down: bfloat16 [8, 12288, 4096], P('expert', 'dp')
The draws below stay inside these ranges and needn't reach their ends.
Inputs may be any that keep to these rules, and one draw needn't show every extreme that they name: `routes`: each token names two different experts. Among the 8 tokens of one block (aligned blocks of tokens, one for each dp index) no expert is named more than 3 times, and some expert reaches 3 in some block.
All inputs are finite; a program needn't handle non-finite values.
Results may differ from the reference program's by a relative error of at most 0.0049.
Values may be sent and summed in bfloat16 or wider, within the bound.
A program may use at most 128 MiB of HBM per device.

```python
import math
import jax
import jax.numpy as jnp
import numpy as np
from jax import lax

D = 4096
FF = 12288
EXPERTS = 8
TOK_DEV = 2
SLOTS = 3
TOKENS = 64
N_DP = 8
N_EXPERT = 4


def shard_levels(own_key, extent, split, smallest, high):
    level, own = 1.0, jax.random.fold_in(own_key, 6)
    for axis_at, parts in split:
        draws = jnp.exp(jax.random.uniform(jax.random.fold_in(own, axis_at), (parts,), jnp.float32, smallest / len(split), high / len(split)))
        level = level * jnp.repeat(draws, extent[axis_at] // parts).reshape([-1 if axis == axis_at else 1 for axis in range(len(extent))])
    return level


def routed_block(key, own, number, rows, number_of, top, bound, lean):
    sequence = jax.random.permutation(key, number_of)
    crowded, common = shares(number_of, rows * top, bound, lean, True), shares(number_of, rows * top, bound, lean, False)
    places = jnp.arange(number_of)

    def named(lengths, turn):
        used = int((lengths > 0).sum())
        fixed = max(1, used // 4)
        passed = fixed + (places - fixed + turn * (used - fixed)) % max(1, number_of - fixed)
        return jnp.zeros((number_of,), jnp.int32).at[sequence[jnp.where(places < fixed, places, passed)]].set(jnp.asarray(lengths, jnp.int32))

    lengths = jnp.where(number % 4 == 0, named(crowded, number // 4), named(common, number - number // 4 - 1))
    mixed = jax.random.permutation(jax.random.fold_in(own, 3), number_of)
    donor, receiver = mixed[0:number_of // 2 * 2:2], mixed[1:number_of // 2 * 2:2]
    room = jnp.minimum(lengths[donor] - 1, bound - lengths[receiver]) // 2
    room = jnp.where((donor == sequence[0]) | (receiver == sequence[0]) | (lengths[receiver] == 0), 0, jnp.maximum(room, 0))
    passed = jax.random.randint(jax.random.fold_in(own, 4), (number_of // 2,), 0, 1 << 20) % (room + 1)
    lengths = lengths.at[donor].add(-passed).at[receiver].add(passed)
    items = jnp.searchsorted(jnp.cumsum(lengths), jnp.arange(rows * top), side="right").astype(jnp.int32)
    listing = items.reshape(top, rows).T
    listing = listing[jax.random.permutation(jax.random.fold_in(own, 1), rows)]
    turn = jax.random.randint(jax.random.fold_in(own, 2), (rows, 1), 0, top)
    return jnp.take_along_axis(listing, (jnp.arange(top)[None, :] + turn) % top, axis=1)


def shares(count, total, limit, lean, full):
    loads = [(1 << 20) // math.isqrt(rank ** lean) + 1 for rank in range(1, count + 1)]
    largest = limit if full else min(limit, max(-(-total // count), total * loads[0] // sum(loads)))
    least = 1 if total - largest >= count - 1 else 0
    holding, surplus = [largest] + [least] * (count - 1), total - largest - least * (count - 1)
    while surplus > 0:
        movable = [i for i in range(1, count) if holding[i] < largest] or [i for i in range(1, count) if holding[i] < limit]
        whole, budget = sum([loads[i] for i in movable]), surplus
        for i in movable:
            extra = min(limit - holding[i], max(1, budget * loads[i] // whole), surplus)
            holding[i] = holding[i] + extra
            surplus = surplus - extra
    return np.array(holding)


def noise(own_key, shape, scale, limit, pieces=(), kind=jnp.bfloat16):
    drawn = scale * jax.random.normal(own_key, shape, jnp.float32)
    if pieces:
        drawn = drawn * shard_levels(own_key, shape, pieces, -0.22, 0.18)
    return jnp.clip(drawn, -limit, limit).astype(kind)


def setup_inputs(seed: int = 0) -> dict:
    streams_of = jax.random.split(jax.random.key(seed), 7)
    out_grad = noise(streams_of[0], (TOKENS, D), 0.05, 0.29882812, ((0, 32),))
    routes_keys = jax.random.split(jax.random.fold_in(streams_of[1], 1), TOKENS // (N_EXPERT * TOK_DEV))
    routes_turns = jax.random.permutation(jax.random.fold_in(streams_of[1], 3), TOKENS // (N_EXPERT * TOK_DEV))
    routes = jax.vmap(lambda own, number: routed_block(jax.random.fold_in(streams_of[1], 2), own, number, N_EXPERT * TOK_DEV, EXPERTS, 2, SLOTS, 1))(routes_keys, routes_turns).reshape((TOKENS, 2))
    gate_values = jnp.clip(0.099609375 + 0.9003906 * jax.random.uniform(streams_of[2], (TOKENS, 2), jnp.float32) ** shard_levels(streams_of[2], (TOKENS, 2), ((0, 32),), -0.2, 0.2), 0.099609375, 1.0).astype(jnp.bfloat16)
    gate_pre = noise(streams_of[3], (EXPERTS, N_DP * SLOTS, FF), 1.0, 6.0, ((0, 4), (2, 8)))
    up_pre = noise(streams_of[4], (EXPERTS, N_DP * SLOTS, FF), 1.0, 6.0, ((0, 4), (2, 8)))
    w_down = noise(streams_of[5], (EXPERTS, FF, D), FF ** -0.5, 0.0546875, ((0, 4), (1, 8)))
    return {"out_grad": out_grad, "routes": routes, "gate_values": gate_values, "gate_pre": gate_pre, "up_pre": up_pre, "w_down": w_down}


def slot_rows(routes):
    flat_routes = routes.reshape(N_DP, -1)
    onehot = (flat_routes[:, :, None] == jnp.arange(EXPERTS, dtype=jnp.int32)[None, None, :]).astype(jnp.int32)
    position = jnp.sum((jnp.cumsum(onehot, axis=1) - 1) * onehot, axis=2)
    slot_row = jnp.arange(N_DP, dtype=jnp.int32)[:, None] * SLOTS + position
    return slot_row.reshape(-1).astype(jnp.int32)


def reference(out_grad, routes, gate_values, gate_pre, up_pre, w_down):
    expert = routes.reshape(-1).astype(jnp.int32)
    slot_row = slot_rows(routes)
    token_index = jnp.repeat(jnp.arange(TOKENS, dtype=jnp.int32), 2)
    dispatched = jnp.zeros((EXPERTS, N_DP * SLOTS, D), jnp.bfloat16).at[expert, slot_row].set(out_grad[token_index])
    slot_gate = jnp.zeros((EXPERTS, N_DP * SLOTS), jnp.bfloat16).at[expert, slot_row].set(gate_values.reshape(-1))

    def per_expert(packed):
        gate_block, up_block, weights, rows_in, gate_row = packed
        projected = jnp.dot(rows_in, weights.T, preferred_element_type=jnp.float32)
        gate_act = gate_block.astype(jnp.float32)
        up_act = up_block.astype(jnp.float32)
        sigmoid_val = jax.nn.sigmoid(gate_act)
        silu_val = gate_act * sigmoid_val
        hidden = silu_val * up_act
        partial_value = jnp.sum(hidden * projected, axis=1)
        scale_col = gate_row.astype(jnp.float32)[:, None]
        weighted = (scale_col * hidden).astype(jnp.bfloat16)
        down_grad = jnp.dot(weighted.T, rows_in, preferred_element_type=jnp.float32).astype(jnp.bfloat16)
        grad_hidden = scale_col * projected
        grad_gate = (grad_hidden * up_act * sigmoid_val * (1.0 + gate_act * (1.0 - sigmoid_val))).astype(jnp.bfloat16)
        grad_up = (grad_hidden * silu_val).astype(jnp.bfloat16)
        return partial_value, grad_gate, grad_up, down_grad

    partial_value, grad_gate_pre, grad_up_pre, grad_down = lax.map(per_expert, (gate_pre, up_pre, w_down, dispatched, slot_gate))
    grad_gates = partial_value[expert, slot_row].reshape(TOKENS, 2)
    return grad_gates, grad_gate_pre, grad_up_pre, grad_down
```

```python
import functools

import jax
import jax.numpy as jnp
from jax import lax
from jax.experimental import pallas as pl
from jax.experimental.pallas import tpu as pltpu
from jax.sharding import PartitionSpec as P

SLOTS = 3


def expert_terms(gate_piece, up_piece, weights, rows_in, gate_row):
    projected = jnp.einsum("erd,efd->erf", rows_in, weights, preferred_element_type=jnp.float32)
    gate_act = gate_piece.astype(jnp.float32)
    up_act = up_piece.astype(jnp.float32)
    sigmoid_val = jax.nn.sigmoid(gate_act)
    silu_val = gate_act * sigmoid_val
    hidden = silu_val * up_act
    partial_value = jnp.sum(hidden * projected, axis=2)
    scale_col = gate_row.astype(jnp.float32)[:, :, None]
    weighted = (scale_col * hidden).astype(jnp.bfloat16)
    down_term = jnp.einsum("erf,erd->efd", weighted, rows_in, preferred_element_type=jnp.float32)
    grad_hidden = scale_col * projected
    grad_gate = (
        grad_hidden * up_act * sigmoid_val * (1.0 + gate_act * (1.0 - sigmoid_val))
    ).astype(jnp.bfloat16)
    grad_up = (grad_hidden * silu_val).astype(jnp.bfloat16)
    return (partial_value, grad_gate, grad_up, down_term)


def general_device(out_grad, routes, gate_values, gate_pre, up_pre, w_down):
    groups = lax.axis_size("expert")
    local_count = gate_pre.shape[0]
    experts = local_count * groups
    tok_count = out_grad.shape[0]
    my_rank = lax.axis_index("expert")
    flat_routes = routes.reshape(-1)
    onehot = (flat_routes[:, None] == jnp.arange(experts, dtype=jnp.int32)[None, :]).astype(
        jnp.int32
    )
    position = jnp.sum((jnp.cumsum(onehot, axis=0) - 1) * onehot, axis=1)
    own_expert = lax.dynamic_slice_in_dim(flat_routes, my_rank * tok_count * 2, tok_count * 2)
    own_position = lax.dynamic_slice_in_dim(position, my_rank * tok_count * 2, tok_count * 2)
    target = own_expert * SLOTS + own_position
    selector = target[:, None] == jnp.arange(experts * SLOTS, dtype=jnp.int32)[None, :]
    picker = selector.astype(jnp.bfloat16).T
    pair_rows = jnp.repeat(out_grad, 2, axis=0)
    send_rows = (
        jnp.dot(picker, pair_rows, preferred_element_type=jnp.float32)
        .astype(jnp.bfloat16)
        .reshape(experts, SLOTS, -1)
    )
    send_gates = (
        jnp.dot(picker, gate_values.reshape(-1, 1), preferred_element_type=jnp.float32)
        .astype(jnp.bfloat16)
        .reshape(experts, SLOTS)
    )
    got_rows, got_gates = (
        lax.all_to_all(send_rows, "expert", split_axis=0, concat_axis=0, tiled=True),
        lax.all_to_all(send_gates, "expert", split_axis=0, concat_axis=0, tiled=True),
    )
    dispatched = jnp.sum(
        got_rows.reshape(groups, local_count, SLOTS, -1).astype(jnp.float32), axis=0
    ).astype(jnp.bfloat16)
    slot_gate = jnp.sum(
        got_gates.reshape(groups, local_count, SLOTS).astype(jnp.float32), axis=0
    ).astype(jnp.bfloat16)
    all_rows, all_gates = (
        lax.all_gather(dispatched, "dp", axis=1, tiled=True),
        lax.all_gather(slot_gate, "dp", axis=1, tiled=True),
    )
    partial_value, grad_gate_pre, grad_up_pre, down_sum = expert_terms(
        gate_pre, up_pre, w_down, all_rows, all_gates
    )
    grad_down = down_sum.astype(jnp.bfloat16)
    own_sums = lax.psum_scatter(partial_value, "dp", scatter_dimension=1, tiled=True)
    score_table = lax.all_gather(own_sums, "expert", axis=0, tiled=True)
    picked = jnp.sum(jnp.where(selector, score_table.reshape(1, -1), 0.0), axis=1)
    grad_gates = picked.reshape(tok_count, 2)
    return (grad_gates, grad_gate_pre, grad_up_pre, grad_down)


LANES = 128
CORES = 2
MESH = pl.DeviceIdType.MESH


def pow2(n):
    return n & (n - 1) == 0


def fused_fits(n_dp, groups, tokens, width, local, rows, hidden):
    if 16 % tokens or n_dp % CORES:
        return False
    split = 16 // tokens
    padded = -(-rows // 16) * 16
    return (
        width % (split * LANES) == 0
        and hidden % 512 == 0
        and local * padded <= LANES
        and pow2(split)
        and pow2(groups)
        and n_dp * groups <= 64
        and rows == n_dp * SLOTS
        and local * hidden * width * 2 <= 32 << 20
    )


def gather_project(
    n_dp, groups, split, local, rows, padded, block,
    payload, gate_pre, up_pre, weights,
    rows_out, gates_out, proj_out, grads_out,
    table, held, sums_own, sums_all,
    load_sem, own_sem, send_z, recv_z, send_c, recv_c, send_p, recv_p, send_s, recv_s,
):
    me_dp, me_z = lax.axis_index("dp"), lax.axis_index("expert")
    total = n_dp * groups
    me = me_dp * groups + me_z
    chips = n_dp // CORES
    chip, core = me_dp // CORES, lax.rem(me_dp, CORES)
    hidden = held.shape[1]
    per = hidden // block
    chunk = payload.shape[1] - LANES

    loads = []
    for e in range(local):
        for b in range(per):
            copy = pltpu.make_async_copy(
                weights.at[e, pl.ds(b * block, block)],
                held.at[e, pl.ds(b * block, block)],
                load_sem.at[e * per + b],
            )
            copy.start()
            loads.append(copy)
    keep = pltpu.make_async_copy(payload, table.at[me], own_sem)
    keep.start()

    barrier = pltpu.get_barrier_semaphore()
    for off in range(1, total):
        other = lax.rem(me + off, total)
        pl.semaphore_signal(
            barrier, inc=1, device_id=(other // groups, lax.rem(other, groups)), device_id_type=MESH
        )
    pl.semaphore_wait(barrier, total - 1)

    sent = []
    first = []
    for dz in range(1, groups):
        copy = pltpu.make_async_remote_copy(
            src_ref=payload,
            dst_ref=table.at[me],
            send_sem=send_z.at[dz],
            recv_sem=recv_z.at[dz],
            device_id=(me_dp, lax.rem(me_z + dz, groups)),
            device_id_type=MESH,
        )
        copy.start()
        first.append(copy)
    sent += first
    keep.wait()
    for copy in first:
        copy.wait_recv()

    def block_copy(dp_index, target, s_sem, r_sem):
        copy = pltpu.make_async_remote_copy(
            src_ref=table.at[pl.ds(dp_index * groups, groups)],
            dst_ref=table.at[pl.ds(dp_index * groups, groups)],
            send_sem=s_sem,
            recv_sem=r_sem,
            device_id=(target, me_z),
            device_id_type=MESH,
        )
        copy.start()
        return copy

    second = []
    for dc in range(1, chips):
        target = lax.rem(chip + dc, chips) * CORES + core
        second.append(block_copy(me_dp, target, send_c.at[dc], recv_c.at[dc]))
    partner = chip * CORES + (1 - core)
    third = [block_copy(me_dp, partner, send_p.at[0], recv_p.at[0])]
    for dc in range(1, chips):
        second[dc - 1].wait_recv()
        source = lax.rem(chip - dc + chips, chips) * CORES + core
        third.append(block_copy(source, partner, send_p.at[dc], recv_p.at[dc]))
    for copy in third:
        copy.wait_recv()
    sent += second + third

    depth = total * 16
    wide = local * padded
    data = table[...].reshape(depth, chunk + LANES)
    meta_low = data[:, chunk:]
    meta = meta_low.astype(jnp.float32)
    row = lax.broadcasted_iota(jnp.int32, (depth, 1), 0)
    piece = (row & (split - 1)).astype(jnp.float32)
    col = lax.broadcasted_iota(jnp.int32, (depth, split * wide), 1).astype(jnp.float32)
    low = (me_z * local).astype(jnp.float32)
    picks = []
    for k in range(2):
        offset = meta[:, 2 * k : 2 * k + 1] - low
        code = piece * wide + offset * padded + meta[:, 2 * k + 1 : 2 * k + 2]
        code = jnp.where((offset >= 0) & (offset < local), code, -1.0)
        picks.append(jnp.where(col == code, 1.0, 0.0))
    either = (picks[0] + picks[1]).T.astype(jnp.bfloat16)
    slots = jnp.dot(either, data[:, :chunk], preferred_element_type=jnp.float32).astype(jnp.bfloat16)
    for c in range(split):
        for e in range(local):
            at = c * wide + e * padded
            rows_out[e, :, c * chunk : (c + 1) * chunk] = slots[at : at + padded]
    scale = jnp.zeros((wide, 1), jnp.float32)
    for k in range(2):
        pick = picks[k][:, :LANES].T.astype(jnp.bfloat16)
        got = jnp.dot(pick, meta_low, preferred_element_type=jnp.float32)
        scale = scale + got[:wide, 4 + k : 5 + k]
    for e in range(local):
        gates_out[e] = jnp.broadcast_to(scale[e * padded : (e + 1) * padded], (padded, LANES))

    lane = lax.broadcasted_iota(jnp.int32, (rows, LANES), 1)
    slot = lax.broadcasted_iota(jnp.int32, (rows, LANES), 0)
    mine = jnp.zeros((1, LANES), jnp.float32)
    for e in range(local):
        part = jnp.zeros((rows, 1), jnp.float32)
        for b in range(per):
            loads[e * per + b].wait()
            span = slice(b * block, (b + 1) * block)
            proj = lax.dot_general(
                rows_out[e], held[e, span], (((1,), (1,)), ((), ())),
                preferred_element_type=jnp.float32,
            )[:rows]
            proj_out[e, :, span] = proj
            gate_act = gate_pre[e, :, span].astype(jnp.float32)
            up_act = up_pre[e, :, span].astype(jnp.float32)
            silu_val = gate_act * jax.nn.sigmoid(gate_act)
            part = part + jnp.sum(silu_val * up_act * proj, axis=1, keepdims=True)
        mine = mine + jnp.sum(
            jnp.where(lane == slot + e * padded, part, 0.0), axis=0, keepdims=True
        )
    sums_own[...] = mine
    sums_all[me] = mine
    last = []
    for off in range(1, total):
        other = lax.rem(me + off, total)
        copy = pltpu.make_async_remote_copy(
            src_ref=sums_own,
            dst_ref=sums_all.at[me],
            send_sem=send_s.at[off],
            recv_sem=recv_s.at[off],
            device_id=(other // groups, lax.rem(other, groups)),
            device_id_type=MESH,
        )
        copy.start()
        last.append(copy)
    for copy in last:
        copy.wait_recv()
    sent += last

    own = payload[:, chunk:].astype(jnp.float32)
    lane_at = lax.broadcasted_iota(jnp.int32, (1, LANES), 1)
    out_row = lax.broadcasted_iota(jnp.int32, grads_out.shape, 0)
    out_col = lax.broadcasted_iota(jnp.int32, grads_out.shape, 1)
    by_group = []
    for z in range(groups):
        acc = sums_all[z]
        for d in range(1, n_dp):
            acc = acc + sums_all[d * groups + z]
        by_group.append(acc)
    result = jnp.zeros(grads_out.shape, jnp.float32)
    for t in range(16 // split):
        for k in range(2):
            expert = own[t * split : t * split + 1, 2 * k : 2 * k + 1]
            spot = own[t * split : t * split + 1, 2 * k + 1 : 2 * k + 2]
            value = jnp.zeros((1, LANES), jnp.float32)
            for z in range(groups):
                offset = expert - z * local
                code = jnp.where((offset >= 0) & (offset < local), offset * padded + spot, -1.0)
                value = value + jnp.where(lane_at.astype(jnp.float32) == code, by_group[z], 0.0)
            value = jnp.sum(value, axis=1, keepdims=True)
            result = jnp.where((out_row == t) & (out_col == k), value, result)
    grads_out[...] = result
    for copy in sent:
        copy.wait_send()


def finish(
    rows, proj, rows_in, gates, gate_pre, up_pre, sums, grad_gate, grad_up, grad_down, grad_sums
):
    grad_sums[...] = sums[...]
    gate_act = gate_pre[0].astype(jnp.float32)
    up_act = up_pre[0].astype(jnp.float32)
    sigmoid_val = jax.nn.sigmoid(gate_act)
    silu_val = gate_act * sigmoid_val
    scale = gates[0, :rows, 0:1]
    grad_hidden = scale * proj[0]
    grad_gate[0] = (
        grad_hidden * up_act * sigmoid_val * (1.0 + gate_act * (1.0 - sigmoid_val))
    ).astype(jnp.bfloat16)
    grad_up[0] = (grad_hidden * silu_val).astype(jnp.bfloat16)
    weighted = scale * (silu_val * up_act)
    fill = rows_in.shape[1] - rows
    if fill:
        weighted = jnp.concatenate(
            [weighted, jnp.zeros((fill, weighted.shape[1]), jnp.float32)], axis=0
        )
    turned = weighted.T.astype(jnp.bfloat16)
    step = 512
    for c in range(0, rows_in.shape[2], step):
        grad_down[0, :, c : c + step] = jnp.dot(
            turned, rows_in[0, :, c : c + step], preferred_element_type=jnp.float32
        ).astype(jnp.bfloat16)


def fused_device(out_grad, routes, gate_values, gate_pre, up_pre, w_down):
    n_dp, groups = lax.axis_size("dp"), lax.axis_size("expert")
    tokens, width = out_grad.shape
    local, rows, hidden = gate_pre.shape
    split = 16 // tokens
    chunk = width // split
    padded = -(-rows // 16) * 16
    block = 512
    total = n_dp * groups
    me_dp, me_z = lax.axis_index("dp"), lax.axis_index("expert")

    flat = routes.reshape(-1)
    count = flat.shape[0]
    earlier = jnp.arange(count)[None, :] < jnp.arange(count)[:, None]
    position = jnp.sum(((flat[:, None] == flat[None, :]) & earlier).astype(jnp.int32), axis=1)
    both = jnp.stack([flat, position + me_dp * SLOTS], axis=1).reshape(groups, tokens, 4)
    pick = (jnp.arange(groups) == me_z)[:, None, None]
    codes = jnp.sum(jnp.where(pick, both, 0), axis=0).astype(jnp.bfloat16)
    meta = jnp.concatenate([codes, gate_values], axis=1)
    meta = jnp.pad(meta, ((0, 0), (0, LANES - 6)))
    meta = jnp.broadcast_to(meta[:, None, :], (tokens, split, LANES)).reshape(16, LANES)
    payload = jnp.concatenate([out_grad.reshape(16, chunk), meta], axis=1)

    vmem = pl.BlockSpec(memory_space=pltpu.VMEM)
    dma = pltpu.SemaphoreType.DMA
    chips = n_dp // CORES
    rows_in, gates, proj, sums = pl.pallas_call(
        functools.partial(
            gather_project, n_dp, groups, split, local, rows, padded, block
        ),
        out_shape=(
            jax.ShapeDtypeStruct((local, padded, width), jnp.bfloat16),
            jax.ShapeDtypeStruct((local, padded, LANES), jnp.float32),
            jax.ShapeDtypeStruct((local, rows, hidden), jnp.float32),
            jax.ShapeDtypeStruct((tokens, 2), jnp.float32),
        ),
        in_specs=[vmem, vmem, vmem, pl.BlockSpec(memory_space=pl.ANY)],
        out_specs=(vmem, vmem, vmem, vmem),
        scratch_shapes=[
            pltpu.VMEM((total, 16, chunk + LANES), jnp.bfloat16),
            pltpu.VMEM((local, hidden, width), jnp.bfloat16),
            pltpu.VMEM((1, LANES), jnp.float32),
            pltpu.VMEM((total, 1, LANES), jnp.float32),
            dma((local * hidden // block,)),
            dma,
            dma((groups,)),
            dma((groups,)),
            dma((chips,)),
            dma((chips,)),
            dma((chips,)),
            dma((chips,)),
            dma((total,)),
            dma((total,)),
        ],
        compiler_params=pltpu.CompilerParams(
            collective_id=0, has_side_effects=True, vmem_limit_bytes=60 << 20
        ),
        name="gather_project",
    )(payload, gate_pre, up_pre, w_down)

    piece = 256
    small = pl.BlockSpec((1, rows, piece), lambda e, b: (e, 0, b))
    grad_gate_pre, grad_up_pre, grad_down, grad_gates = pl.pallas_call(
        functools.partial(finish, rows),
        grid=(local, hidden // piece),
        out_shape=(
            jax.ShapeDtypeStruct(gate_pre.shape, jnp.bfloat16),
            jax.ShapeDtypeStruct(gate_pre.shape, jnp.bfloat16),
            jax.ShapeDtypeStruct(w_down.shape, jnp.bfloat16),
            jax.ShapeDtypeStruct((tokens, 2), jnp.float32),
        ),
        in_specs=[
            small,
            pl.BlockSpec((1, padded, width), lambda e, b: (e, 0, 0)),
            pl.BlockSpec((1, padded, LANES), lambda e, b: (e, 0, 0)),
            small,
            small,
            pl.BlockSpec((tokens, 2), lambda e, b: (0, 0)),
        ],
        out_specs=(
            small,
            small,
            pl.BlockSpec((1, piece, width), lambda e, b: (e, b, 0)),
            pl.BlockSpec((tokens, 2), lambda e, b: (0, 0)),
        ),
        compiler_params=pltpu.CompilerParams(vmem_limit_bytes=60 << 20),
        name="finish",
    )(proj, rows_in, gates, gate_pre, up_pre, sums)
    return grad_gates, grad_gate_pre, grad_up_pre, grad_down


def per_device(out_grad, routes, gate_values, gate_pre, up_pre, w_down):
    fits = fused_fits(
        lax.axis_size("dp"), lax.axis_size("expert"), *out_grad.shape, *gate_pre.shape
    )
    chosen = fused_device if fits else general_device
    return chosen(out_grad, routes, gate_values, gate_pre, up_pre, w_down)


def solution(mesh):
    return jax.shard_map(
        per_device,
        mesh=mesh,
        in_specs=(
            P(("dp", "expert"), None),
            P("dp", None),
            P(("dp", "expert"), None),
            P("expert", None, "dp"),
            P("expert", None, "dp"),
            P("expert", "dp", None),
        ),
        out_specs=(
            P(("dp", "expert"), None),
            P("expert", None, "dp"),
            P("expert", None, "dp"),
            P("expert", "dp", None),
        ),
        check_vma=False,
    )
```
